32 devices in a mesh: row: 8 (over z, core), col: 4 (over y, x).
Axes of the slice: x: 2, y: 2, z: 4, core: 2. Of those that a mesh axis runs over, the one named last changes fastest.
Arguments:
- tokens: bfloat16 [12288, 2048], P('row', 'col'), may hold values from -6 to 6
- weight_query: bfloat16 [2048, 2048], P('row', 'col'), may hold values from -0.125 to 0.125
- weight_key: bfloat16 [2048, 2048], P('row', 'col'), may hold values from -0.125 to 0.125
- weight_value: bfloat16 [2048, 2048], P('row', 'col'), may hold values from -0.125 to 0.125
- weight_output: bfloat16 [2048, 2048], P('col', 'row'), may hold values from -0.125 to 0.125
- weight_gate: bfloat16 [2048, 8192], P('row', 'col'), may hold values from -0.125 to 0.125
- weight_up: bfloat16 [2048, 8192], P('row', 'col'), may hold values from -0.125 to 0.125
- weight_down: bfloat16 [8192, 2048], P('col', 'row'), may hold values from -0.0625 to 0.0625
- gain_query: float32 [2048], P('col'), may hold values from 0.25 to 1.75
- gain_key: float32 [2048], P('col'), may hold values from 0.25 to 1.75
- gain_attention: float32 [2048], replicated, may hold values from 0.5 to 1.5
- gain_feedforward: float32 [2048], replicated, may hold values from 0.5 to 1.5
- positions: int32 [12288], P('row'), may hold values from 0 to 1279, as said below
- segments: int32 [12288], P('row'), may hold values from 0 to 2, as said below
- cotangent: bfloat16 [12288, 2048], P('row', 'col'), may hold values from -6 to 6
Outputs:
- activations: bfloat16 [12288, 2048], P('row', 'col')
- input_grad: float32 [12288, 2048], P('row', 'col')
- query_weight_grad: float32 [2048, 2048], P('row', 'col')
- key_weight_grad: float32 [2048, 2048], P('row', 'col')
- value_weight_grad: float32 [2048, 2048], P('row', 'col')
- output_weight_grad: float32 [2048, 2048], P('col', 'row')
- gate_weight_grad: float32 [2048, 8192], P('row', 'col')
- up_weight_grad: float32 [2048, 8192], P('row', 'col')
- down_weight_grad: float32 [8192, 2048], P('col', 'row')
- query_gain_grad: float32 [2048], P('col')
- key_gain_grad: float32 [2048], P('col')
- attention_gain_grad: float32 [2048], replicated
- feedforward_gain_grad: float32 [2048], replicated
The draws below stay inside these ranges and needn't reach their ends.
Inputs may be any that keep to these rules, and one draw needn't show every extreme that they name: The 1536 rows of each index of row form one group: the prompt's 1024 rows are consecutive with segment 0 and positions 0 to 1023; each continuation has 256 consecutive rows, one segment of 1 to 2 (each once a group) and positions 1024 to 1279 in order; the prompt lies before, between or after whole continuations. `segments`: segment ids of the layout described for positions.
All inputs are finite; a program needn't handle non-finite values.
Results may differ from the reference program's by a relative error of at most 0.02.
Values may be sent and summed in bfloat16 or wider, within the bound.
A program may use at most 320 MiB of HBM per device.

```python
import jax
import jax.numpy as jnp
from jax import lax

D = 2048
HEADS = 16
HD = 128
FF = 8192
PROMPT = 1024
CLEN = 256
CONTS = 2
TOK_ROW = 1536
GROUPS = 8
TOKENS = 12288


def group_layout(key):

    def one_group(group_index):
        group_key = jax.random.fold_in(jax.random.fold_in(key, 7), group_index)
        place_key, order_key = jax.random.split(group_key)
        before = jax.random.randint(place_key, (), 0, CONTS + 1) * CLEN
        labels = jax.random.permutation(order_key, CONTS).astype(jnp.int32) + 1
        offsets = jnp.arange(TOK_ROW, dtype=jnp.int32)
        in_prompt = (offsets >= before) & (offsets < before + PROMPT)
        outside = jnp.where(offsets < before, offsets, offsets - PROMPT)
        slot_index = jnp.clip(outside // CLEN, 0, CONTS - 1)
        segment_ids = jnp.where(in_prompt, 0, labels[slot_index])
        position_ids = jnp.where(in_prompt, offsets - before, PROMPT + outside % CLEN)
        return (segment_ids.astype(jnp.int32), position_ids.astype(jnp.int32))
    segment_ids, position_ids = jax.vmap(one_group)(jnp.arange(GROUPS, dtype=jnp.int32))
    return (segment_ids.reshape(TOKENS), position_ids.reshape(TOKENS))


def draw_positions(key, part):
    return group_layout(key)[1]


def draw_segments(key, part):
    return group_layout(key)[0]


def level_of(own_key, dims, shards, smallest, high):
    level = 1.0
    for axis_at, blocks in shards:
        draws = jax.random.uniform(jax.random.fold_in(jax.random.fold_in(own_key, 6), axis_at), (blocks,), jnp.float32, smallest / len(shards), high / len(shards))
        level = level * jnp.repeat(jnp.exp(draws), dims[axis_at] // blocks).reshape((-1,) + (1,) * (len(dims) - 1 - axis_at))
    return level


def centred(rng, extent, scale, limit, pieces=(), kind=jnp.bfloat16):
    drawn = jax.random.normal(rng, extent, jnp.float32) * scale
    if len(pieces) > 0:
        drawn = level_of(rng, extent, pieces, -0.22, 0.18) * drawn
    return jnp.clip(drawn, min=-limit, max=limit).astype(kind)


def setup_inputs(seed: int = 0) -> dict:
    arg_keys = jax.random.split(jax.random.key(seed), 16)
    tokens = centred(arg_keys[0], (TOKENS, D), 1.0, 6.0, ((0, 8), (1, 4)))
    weight_query = centred(arg_keys[1], (D, D), D ** -0.5, 0.125, ((0, 8), (1, 4)))
    weight_key = centred(arg_keys[2], (D, D), D ** -0.5, 0.125, ((0, 8), (1, 4)))
    weight_value = centred(arg_keys[3], (D, D), D ** -0.5, 0.125, ((0, 8), (1, 4)))
    weight_output = centred(arg_keys[4], (D, D), D ** -0.5, 0.125, ((0, 4), (1, 8)))
    weight_gate = centred(arg_keys[5], (D, FF), D ** -0.5, 0.125, ((0, 8), (1, 4)))
    weight_up = centred(arg_keys[6], (D, FF), D ** -0.5, 0.125, ((0, 8), (1, 4)))
    weight_down = centred(arg_keys[7], (FF, D), FF ** -0.5, 0.0625, ((0, 4), (1, 8)))
    gain_query = jnp.clip(1.0 + 0.15 * jax.random.normal(arg_keys[8], (D,), jnp.float32), 0.25, 1.75)
    gain_key = jnp.clip(1.0 + 0.15 * jax.random.normal(arg_keys[9], (D,), jnp.float32), 0.25, 1.75)
    gain_attention = jnp.clip(1.0 + 0.1 * jax.random.normal(arg_keys[10], (D,), jnp.float32), 0.5, 1.5)
    gain_feedforward = jnp.clip(1.0 + 0.1 * jax.random.normal(arg_keys[11], (D,), jnp.float32), 0.5, 1.5)
    positions = draw_positions(jax.random.fold_in(arg_keys[15], 71), 0)
    segments = draw_segments(jax.random.fold_in(arg_keys[15], 71), 0)
    cotangent = centred(arg_keys[14], (TOKENS, D), 1.0, 6.0, ((0, 8), (1, 4)))
    return {"tokens": tokens, "weight_query": weight_query, "weight_key": weight_key, "weight_value": weight_value, "weight_output": weight_output, "weight_gate": weight_gate, "weight_up": weight_up, "weight_down": weight_down, "gain_query": gain_query, "gain_key": gain_key, "gain_attention": gain_attention, "gain_feedforward": gain_feedforward, "positions": positions, "segments": segments, "cotangent": cotangent}


EPSILON = 1e-06
ROPE_BASE = 500000.0
NEGATIVE = -1e+30

@jax.custom_vjp
def low(v):
    return lax.optimization_barrier(v.astype(jnp.bfloat16)).astype(jnp.float32)

@jax.custom_vjp
def low_back(v):
    return v

def low_keep(v):
    return (low(v), None)

def low_pass(kept, grad):
    return (grad,)

def back_keep(v):
    return (v, None)

def back_low(kept, grad):
    return (low(grad),)
low.defvjp(low_keep, low_pass)
low_back.defvjp(back_keep, back_low)

def matmul_high(left, right):
    return jnp.dot(left, right, precision=lax.Precision.HIGHEST)

def normalize(values):
    return values * lax.rsqrt(lax.optimization_barrier(jnp.mean(values * values, axis=-1, keepdims=True)) + EPSILON)

def rotary(values, position_ids):
    half_dim = HD // 2
    inverse = ROPE_BASE ** (-(jnp.arange(half_dim).astype(jnp.float32) * 2.0) / HD)
    angles = position_ids.astype(jnp.float32)[:, None] * inverse[None, :]
    cosine_table = jnp.cos(angles)[:, None, :]
    sine_table = jnp.sin(angles)[:, None, :]
    shaped = values.reshape(values.shape[0], HEADS, HD)
    lower_half = shaped[..., :half_dim]
    upper_half = shaped[..., half_dim:]
    rotated = jnp.concatenate([lower_half * cosine_table - upper_half * sine_table, upper_half * cosine_table + lower_half * sine_table], axis=-1)
    return rotated.reshape(values.shape[0], HEADS * HD)

def group_attention(packed):
    query_rows, key_rows, value_rows, segment_ids, position_ids = packed
    query_heads = query_rows.reshape(TOK_ROW, HEADS, HD)
    key_heads = key_rows.reshape(TOK_ROW, HEADS, HD)
    value_heads = value_rows.reshape(TOK_ROW, HEADS, HD)
    scores = jnp.einsum('qhd,khd->hqk', query_heads, key_heads, precision=lax.Precision.HIGHEST) * HD ** (-0.5)
    scores = low_back(scores)
    shared = (segment_ids[None, :] == 0) | (segment_ids[None, :] == segment_ids[:, None])
    allowed = shared & (position_ids[None, :] <= position_ids[:, None])
    scores = jnp.where(allowed[None], scores, NEGATIVE)
    attn_probs = jax.nn.softmax(scores, axis=-1)
    context = jnp.einsum('hqk,khd->qhd', low(attn_probs), value_heads, precision=lax.Precision.HIGHEST)
    return context.reshape(TOK_ROW, HEADS * HD)

def reference(tokens, weight_query, weight_key, weight_value, weight_output, weight_gate, weight_up, weight_down, gain_query, gain_key, gain_attention, gain_feedforward, positions, segments, cotangent):

    def forward(features, query_matrix, key_matrix, value_matrix, output_matrix, gate_matrix, up_matrix, down_matrix, query_gain, key_gain, attention_gain, feedforward_gain):
        query_raw = low_back(matmul_high(features, query_matrix))
        key_raw = low_back(matmul_high(features, key_matrix))
        value_rows = low(low_back(matmul_high(features, value_matrix)))
        query_rot = low(rotary(normalize(query_raw) * query_gain, positions))
        key_rot = low(rotary(normalize(key_raw) * key_gain, positions))
        context = lax.map(jax.checkpoint(group_attention), (query_rot.reshape(GROUPS, TOK_ROW, D), key_rot.reshape(GROUPS, TOK_ROW, D), value_rows.reshape(GROUPS, TOK_ROW, D), segments.reshape(GROUPS, TOK_ROW), positions.reshape(GROUPS, TOK_ROW)))
        context = low(low_back(context.reshape(TOKENS, D)))
        attention_out = low_back(matmul_high(context, output_matrix))
        hidden_state = features + normalize(attention_out) * attention_gain
        hidden_low = low(hidden_state)
        gate = low_back(matmul_high(hidden_low, gate_matrix))
        up_rows = low_back(matmul_high(hidden_low, up_matrix))
        activated = low(jax.nn.silu(gate) * up_rows)
        feedforward_out = low_back(matmul_high(activated, down_matrix))
        return hidden_state + normalize(feedforward_out) * feedforward_gain
    inputs = (tokens.astype(jnp.float32), weight_query.astype(jnp.float32), weight_key.astype(jnp.float32), weight_value.astype(jnp.float32), weight_output.astype(jnp.float32), weight_gate.astype(jnp.float32), weight_up.astype(jnp.float32), weight_down.astype(jnp.float32), gain_query.astype(jnp.float32), gain_key.astype(jnp.float32), gain_attention.astype(jnp.float32), gain_feedforward.astype(jnp.float32))
    result, pullback = jax.vjp(forward, *inputs)
    grads = pullback(cotangent.astype(jnp.float32))
    return (result.astype(jnp.bfloat16), grads[0], grads[1], grads[2], grads[3], grads[4], grads[5], grads[6], grads[7], grads[8], grads[9], grads[10], grads[11])
```

```python
import jax
import jax.numpy as jnp
from jax import lax
from jax.sharding import PartitionSpec as P

D = 2048
HD = 128


EPSILON = 1e-06
ROPE_BASE = 500000.0
NEGATIVE = -1e30
block_limit = 512


def times_plain(left, right):
    return jnp.dot(left, right, preferred_element_type=jnp.float32)


def times_transposed(left, right):
    return lax.dot_general(
        left, right, (((1,), (1,)), ((), ())), preferred_element_type=jnp.float32
    )


def transposed_times(left, right):
    return lax.dot_general(
        left, right, (((0,), (0,)), ((), ())), preferred_element_type=jnp.float32
    )


def rotation(positions):
    half_dim = HD // 2
    inverse = ROPE_BASE ** (-(jnp.arange(half_dim).astype(jnp.float32) * 2.0) / HD)
    angles = positions.astype(jnp.float32)[:, None] * inverse[None, :]
    return (jnp.cos(angles), jnp.sin(angles))


def rotate(values, cosine_table, sine_table, direction):
    row_count, local_width = values.shape
    local_heads = local_width // HD
    half_dim = HD // 2
    shaped = values.reshape(row_count, local_heads, HD)
    lower_half = shaped[..., :half_dim]
    upper_half = shaped[..., half_dim:]
    cosine_rows = cosine_table[:, None, :]
    sine_rows = direction * sine_table[:, None, :]
    rotated = jnp.concatenate(
        [
            lower_half * cosine_rows - upper_half * sine_rows,
            upper_half * cosine_rows + lower_half * sine_rows,
        ],
        axis=-1,
    )
    return rotated.reshape(row_count, local_width)


def allowed_pairs(segment_block, position_block, segments, positions):
    shared = (segments[None, :] == 0) | (segments[None, :] == segment_block[:, None])
    return shared & (positions[None, :] <= position_block[:, None])


def norm_back(incoming, values, norm_scale, gain_vector):
    scaled = gain_vector * incoming
    inner_mean = jnp.mean(scaled * values, axis=-1, keepdims=True)
    grad_values = norm_scale * scaled - values * norm_scale * norm_scale * norm_scale * inner_mean
    return (grad_values, jnp.sum(incoming * values * norm_scale, axis=0))


def spread_share(values, start):
    return lax.dynamic_update_slice_in_dim(jnp.zeros((D,), jnp.float32), values, start, 0)


def attend(query_rot, key_rot, value_low, segments, positions):
    row_count, local_width = query_rot.shape
    local_heads = local_width // HD
    block_rows = min(block_limit, row_count)
    blocks = row_count // block_rows
    key_heads = key_rot.reshape(row_count, local_heads, HD)
    value_heads = value_low.reshape(row_count, local_heads, HD)

    def one_block(packed):
        query_block, segment_block, position_block = packed
        query_heads = query_block.reshape(block_rows, local_heads, HD)
        scores = jnp.einsum(
            "qhd,khd->hqk", query_heads, key_heads, preferred_element_type=jnp.float32
        ) * HD ** (-0.5)
        allowed = allowed_pairs(segment_block, position_block, segments, positions)
        scores = jnp.where(allowed[None], scores, NEGATIVE)
        row_max = jnp.max(scores, axis=-1, keepdims=True)
        exponent = jnp.exp(scores - row_max)
        row_total = jnp.sum(exponent, axis=-1, keepdims=True)
        attn_probs = exponent / row_total
        context = jnp.einsum(
            "hqk,khd->qhd",
            attn_probs.astype(jnp.bfloat16),
            value_heads,
            preferred_element_type=jnp.float32,
        )
        return (context.reshape(block_rows, local_width), (row_max + jnp.log(row_total))[..., 0])

    context, log_norm = lax.map(
        one_block,
        (
            query_rot.reshape(blocks, block_rows, local_width),
            segments.reshape(blocks, block_rows),
            positions.reshape(blocks, block_rows),
        ),
    )
    return (context.reshape(row_count, local_width), log_norm)


def attend_back(query_rot, key_rot, value_low, context_grad, log_norm, segments, positions):
    row_count, local_width = query_rot.shape
    local_heads = local_width // HD
    block_rows = min(block_limit, row_count)
    blocks = row_count // block_rows
    scale_factor = HD ** (-0.5)
    key_heads = key_rot.reshape(row_count, local_heads, HD)
    value_heads = value_low.reshape(row_count, local_heads, HD)

    def one_block(carry, packed):
        key_total, value_total = carry
        query_block, grad_block, norm_block, segment_block, position_block = packed
        query_heads = query_block.reshape(block_rows, local_heads, HD)
        grad_heads = grad_block.reshape(block_rows, local_heads, HD)
        scores = (
            jnp.einsum("qhd,khd->hqk", query_heads, key_heads, preferred_element_type=jnp.float32)
            * scale_factor
        )
        allowed = allowed_pairs(segment_block, position_block, segments, positions)
        scores = jnp.where(allowed[None], scores, NEGATIVE)
        attn_probs = jnp.exp(scores - norm_block[..., None])
        prob_grad = jnp.einsum(
            "qhd,khd->hqk", grad_heads, value_heads, preferred_element_type=jnp.float32
        )
        delta_sum = jnp.sum(attn_probs * prob_grad, axis=-1, keepdims=True)
        score_grad = (attn_probs * (prob_grad - delta_sum)).astype(jnp.bfloat16)
        query_grad = (
            jnp.einsum("hqk,khd->qhd", score_grad, key_heads, preferred_element_type=jnp.float32)
            * scale_factor
        )
        key_total = (
            key_total
            + jnp.einsum(
                "hqk,qhd->khd", score_grad, query_heads, preferred_element_type=jnp.float32
            )
            * scale_factor
        )
        value_total = value_total + jnp.einsum(
            "hqk,qhd->khd",
            attn_probs.astype(jnp.bfloat16),
            grad_heads,
            preferred_element_type=jnp.float32,
        )
        return ((key_total, value_total), query_grad.reshape(block_rows, local_width))

    zeros_heads = jnp.zeros((row_count, local_heads, HD), jnp.float32)
    packed = (
        query_rot.reshape(blocks, block_rows, local_width),
        context_grad.reshape(blocks, block_rows, local_width),
        log_norm,
        segments.reshape(blocks, block_rows),
        positions.reshape(blocks, block_rows),
    )
    (key_grad, value_grad), query_grad = lax.scan(one_block, (zeros_heads, zeros_heads), packed)
    return (
        query_grad.reshape(row_count, local_width),
        key_grad.reshape(row_count, local_width),
        value_grad.reshape(row_count, local_width),
    )


def swap(values, distance, count):
    pairs = [(at, at ^ distance) for at in range(count)]
    return lax.ppermute(values, "col", pairs)


def exchange(pieces, count):
    return [pieces[0]] + [swap(pieces[d], d, count) for d in range(1, count)]


def spread(values, count):
    return [values] + [swap(values, d, count) for d in range(1, count)]


def in_order(pieces, me, axis):
    pieces = list(pieces)
    count = len(pieces)
    bit = 1
    while bit < count:
        chosen = (me & bit) != 0
        pieces = [
            jnp.where(chosen, pieces[at ^ bit], pieces[at]) for at in range(count)
        ]
        bit *= 2
    return jnp.concatenate(pieces, axis=axis)


def total_over_col(values, count):
    got = spread(values, count)
    total = got[0]
    for piece in got[1:]:
        total = total + piece
    return total


def owned_sum(pieces, count):
    got = exchange([pieces[0]] + [p.astype(jnp.bfloat16) for p in pieces[1:]], count)
    total = got[0]
    for piece in got[1:]:
        total = total + piece.astype(jnp.float32)
    return total


def body(
    tokens,
    weight_query,
    weight_key,
    weight_value,
    weight_output,
    weight_gate,
    weight_up,
    weight_down,
    gain_query,
    gain_key,
    gain_attention,
    gain_feedforward,
    positions,
    segments,
    cotangent,
):
    row_count, col_width = tokens.shape
    count = D // col_width
    own_rows = row_count // count
    me = lax.axis_index("col")
    col_start = me * col_width

    def rows_of(values, d):
        return lax.dynamic_slice_in_dim(values, (me ^ d) * own_rows, own_rows, 0)

    def cols_of(values, d):
        return lax.dynamic_slice_in_dim(values, (me ^ d) * col_width, col_width, 1)

    hidden_width = weight_gate.shape[1]

    def block(values, d):
        return values[d * own_rows : (d + 1) * own_rows]

    features = in_order(spread(tokens, count), me, 1)
    qkv_matrix = lax.all_gather(
        jnp.concatenate([weight_query, weight_key, weight_value], axis=1), "row", axis=0, tiled=True
    )
    output_matrix = lax.all_gather(weight_output, "row", axis=1, tiled=True)
    gate_matrix = lax.all_gather(weight_gate, "row", axis=0, tiled=True)
    up_matrix = lax.all_gather(weight_up, "row", axis=0, tiled=True)
    down_matrix = lax.all_gather(weight_down, "row", axis=1, tiled=True)

    qkv = times_plain(features, qkv_matrix)
    query_raw = qkv[:, :col_width]
    key_raw = qkv[:, col_width : 2 * col_width]
    value_low = qkv[:, 2 * col_width :].astype(jnp.bfloat16)
    square_sums = total_over_col(
        jnp.stack([jnp.sum(query_raw * query_raw, axis=-1), jnp.sum(key_raw * key_raw, axis=-1)]),
        count,
    )
    query_scale = lax.rsqrt(square_sums[0] / D + EPSILON)[:, None]
    key_scale = lax.rsqrt(square_sums[1] / D + EPSILON)[:, None]
    cosine_table, sine_table = rotation(positions)
    query_rot = rotate(query_raw * query_scale * gain_query, cosine_table, sine_table, 1.0).astype(
        jnp.bfloat16
    )
    key_rot = rotate(key_raw * key_scale * gain_key, cosine_table, sine_table, 1.0).astype(
        jnp.bfloat16
    )
    context, log_norm = attend(query_rot, key_rot, value_low, segments, positions)
    context_low = context.astype(jnp.bfloat16)
    attention_out = owned_sum(
        [times_plain(rows_of(context_low, d), output_matrix) for d in range(count)], count
    )
    attention_scale = lax.rsqrt(
        jnp.mean(attention_out * attention_out, axis=-1, keepdims=True) + EPSILON
    )
    hidden_state = (
        rows_of(features, 0).astype(jnp.float32) + attention_out * attention_scale * gain_attention
    )
    hidden_low = jnp.concatenate(spread(hidden_state.astype(jnp.bfloat16), count), axis=0)
    gate = times_plain(hidden_low, gate_matrix)
    up_rows = times_plain(hidden_low, up_matrix)
    sigmoid_gate = jax.nn.sigmoid(gate)
    silu_gate = gate * sigmoid_gate
    activated = (silu_gate * up_rows).astype(jnp.bfloat16)
    feedforward_out = owned_sum(
        [times_plain(block(activated, d), down_matrix) for d in range(count)], count
    )
    feedforward_scale = lax.rsqrt(
        jnp.mean(feedforward_out * feedforward_out, axis=-1, keepdims=True) + EPSILON
    )
    result = (
        hidden_state + feedforward_out * feedforward_scale * gain_feedforward
    ).astype(jnp.bfloat16)
    activations = in_order(exchange([cols_of(result, d) for d in range(count)], count), me, 0)
    upstream = in_order(
        exchange([rows_of(cotangent, d) for d in range(count)], count), me, 1
    ).astype(jnp.float32)
    feedforward_own_grad, feedforward_gain_part = norm_back(
        upstream, feedforward_out, feedforward_scale, gain_feedforward
    )
    feedforward_grad = jnp.concatenate(
        spread(feedforward_own_grad.astype(jnp.bfloat16), count), axis=0
    )
    down_weight_part = transposed_times(activated, feedforward_grad).astype(jnp.bfloat16)
    activated_grad = times_transposed(feedforward_grad, down_matrix)
    gate_grad = (
        activated_grad * up_rows * sigmoid_gate * (1.0 + gate * (1.0 - sigmoid_gate))
    ).astype(jnp.bfloat16)
    up_grad = (activated_grad * silu_gate).astype(jnp.bfloat16)
    hidden_grad = (
        owned_sum(
            [
                times_transposed(block(gate_grad, d), gate_matrix)
                + times_transposed(block(up_grad, d), up_matrix)
                for d in range(count)
            ],
            count,
        )
        + upstream
    )
    gate_weight_part = transposed_times(hidden_low, gate_grad).astype(jnp.bfloat16)
    up_weight_part = transposed_times(hidden_low, up_grad).astype(jnp.bfloat16)
    attention_own_grad, attention_gain_part = norm_back(
        hidden_grad, attention_out, attention_scale, gain_attention
    )
    attention_grad = in_order(spread(attention_own_grad.astype(jnp.bfloat16), count), me, 0)
    residual_low = hidden_grad.astype(jnp.bfloat16)
    residual_grad = in_order(
        exchange([cols_of(residual_low, d) for d in range(count)], count), me, 0
    ).astype(jnp.float32)
    context_grad = times_transposed(attention_grad, output_matrix).astype(jnp.bfloat16)
    output_weight_part = transposed_times(context_low, attention_grad).astype(jnp.bfloat16)
    query_rot_grad, key_rot_grad, value_grad = attend_back(
        query_rot, key_rot, value_low, context_grad, log_norm, segments, positions
    )
    value_grad = value_grad.astype(jnp.bfloat16)
    query_norm_grad = rotate(query_rot_grad, cosine_table, sine_table, -1.0)
    key_norm_grad = rotate(key_rot_grad, cosine_table, sine_table, -1.0)
    query_scaled = gain_query * query_norm_grad
    key_scaled = gain_key * key_norm_grad
    inner_sums = total_over_col(
        jnp.stack(
            [jnp.sum(query_scaled * query_raw, axis=-1), jnp.sum(key_scaled * key_raw, axis=-1)]
        ),
        count,
    )
    query_raw_grad = (
        query_scale * query_scaled
        - query_raw * query_scale * query_scale * query_scale * (inner_sums[0] / D)[:, None]
    ).astype(jnp.bfloat16)
    key_raw_grad = (
        key_scale * key_scaled
        - key_raw * key_scale * key_scale * key_scale * (inner_sums[1] / D)[:, None]
    ).astype(jnp.bfloat16)
    query_gain_part = jnp.sum(query_norm_grad * query_raw * query_scale, axis=0)
    key_gain_part = jnp.sum(key_norm_grad * key_raw * key_scale, axis=0)
    qkv_grad = jnp.concatenate([query_raw_grad, key_raw_grad, value_grad], axis=1)
    qkv_weight_part = transposed_times(features, qkv_grad).astype(jnp.bfloat16)
    input_grad = (
        owned_sum(
            [
                times_transposed(
                    qkv_grad,
                    lax.dynamic_slice_in_dim(qkv_matrix, (me ^ d) * col_width, col_width, 0),
                )
                for d in range(count)
            ],
            count,
        )
        + residual_grad
    )

    def share_rows(values, axis):
        return lax.psum_scatter(values, "row", scatter_dimension=axis, tiled=True).astype(
            jnp.float32
        )

    down_weight_grad = share_rows(down_weight_part, 1)
    gate_weight_grad = share_rows(gate_weight_part, 0)
    up_weight_grad = share_rows(up_weight_part, 0)
    output_weight_grad = share_rows(output_weight_part, 1)
    qkv_weight_grad = share_rows(qkv_weight_part, 0)
    gain_totals = lax.psum(
        (
            spread_share(query_gain_part, col_start),
            spread_share(key_gain_part, col_start),
            attention_gain_part,
            feedforward_gain_part,
        ),
        ("row", "col"),
    )
    query_gain_grad = lax.dynamic_slice_in_dim(gain_totals[0], col_start, col_width, 0)
    key_gain_grad = lax.dynamic_slice_in_dim(gain_totals[1], col_start, col_width, 0)
    return (
        activations,
        input_grad,
        qkv_weight_grad[:, :col_width],
        qkv_weight_grad[:, col_width : 2 * col_width],
        qkv_weight_grad[:, 2 * col_width :],
        output_weight_grad,
        gate_weight_grad,
        up_weight_grad,
        down_weight_grad,
        query_gain_grad,
        key_gain_grad,
        gain_totals[2],
        gain_totals[3],
    )


def solution(mesh):
    in_specs = (
        P("row", "col"),
        P("row", "col"),
        P("row", "col"),
        P("row", "col"),
        P("col", "row"),
        P("row", "col"),
        P("row", "col"),
        P("col", "row"),
        P("col"),
        P("col"),
        P(),
        P(),
        P("row"),
        P("row"),
        P("row", "col"),
    )
    out_specs = (
        P("row", "col"),
        P("row", "col"),
        P("row", "col"),
        P("row", "col"),
        P("row", "col"),
        P("col", "row"),
        P("row", "col"),
        P("row", "col"),
        P("col", "row"),
        P("col"),
        P("col"),
        P(),
        P(),
    )
    return jax.shard_map(body, mesh=mesh, in_specs=in_specs, out_specs=out_specs, check_vma=False)
```

```python
import jax
import jax.numpy as jnp
from jax import lax
from jax.experimental import pallas as pl
from jax.experimental.pallas import tpu as pltpu
from jax.sharding import PartitionSpec as P

D = 2048
HD = 128


EPSILON = 1e-06
ROPE_BASE = 500000.0
NEGATIVE = -1e30


def times_plain(left, right):
    return jnp.dot(left, right, preferred_element_type=jnp.float32)


def times_transposed(left, right):
    return lax.dot_general(
        left, right, (((1,), (1,)), ((), ())), preferred_element_type=jnp.float32
    )


def transposed_times(left, right):
    return lax.dot_general(
        left, right, (((0,), (0,)), ((), ())), preferred_element_type=jnp.float32
    )


def rotation(positions):
    half_dim = HD // 2
    inverse = ROPE_BASE ** (-(jnp.arange(half_dim).astype(jnp.float32) * 2.0) / HD)
    angles = positions.astype(jnp.float32)[:, None] * inverse[None, :]
    cosine, sine = jnp.cos(angles), jnp.sin(angles)
    return (
        jnp.concatenate([cosine, cosine], axis=1),
        jnp.concatenate([-sine, sine], axis=1),
    )


def norm_back(incoming, values, norm_scale, gain_vector):
    scaled = gain_vector * incoming
    inner_mean = jnp.mean(scaled * values, axis=-1, keepdims=True)
    grad_values = norm_scale * scaled - values * norm_scale * norm_scale * norm_scale * inner_mean
    return (grad_values, jnp.sum(incoming * values * norm_scale, axis=0))


def spread_share(values, start):
    return lax.dynamic_update_slice_in_dim(jnp.zeros((D,), jnp.float32), values, start, 0)


PROMPT = 1024
CLEN = 256
LOG2_E = 1.4426950408889634
kernel_vmem = 40 * 1024 * 1024


def turn(values, cosine, sine):
    return values * cosine + pltpu.roll(values, HD // 2, 1) * sine


def block_plan(start, rows):
    plan = [(start + at, at) for at in range(0, PROMPT, CLEN)]
    for at in range(0, rows - PROMPT, CLEN):
        plan.append((jnp.where(at < start, at, at + PROMPT), PROMPT))
    return [(pl.multiple_of(first, CLEN), seen) for first, seen in plan]


def diagonal():
    shape = (CLEN, CLEN)
    return lax.broadcasted_iota(jnp.int32, shape, 1) <= lax.broadcasted_iota(jnp.int32, shape, 0)


def attend_kernel(
    start_ref, q_ref, k_ref, v_ref, scale_ref, gain_q_ref, gain_k_ref, cos_ref, sin_ref,
    qr_ref, kr_ref, vl_ref, ctx_ref, norm_ref,
):
    rows = q_ref.shape[0]
    factor = HD ** (-0.5) * LOG2_E
    for at in range(0, rows, CLEN):
        part = pl.ds(at, CLEN)
        cosine, sine = cos_ref[part], sin_ref[part]
        scales = scale_ref[part]
        query = q_ref[part] * scales[:, 0:1] * gain_q_ref[...]
        key = k_ref[part] * scales[:, 1:2] * gain_k_ref[...]
        qr_ref[part] = turn(query, cosine, sine).astype(jnp.bfloat16)
        kr_ref[part] = turn(key, cosine, sine).astype(jnp.bfloat16)
        vl_ref[part] = v_ref[part].astype(jnp.bfloat16)
    start = pl.multiple_of(start_ref[0], CLEN)
    mask = diagonal()
    for first, seen in block_plan(start, rows):
        own = pl.ds(first, CLEN)
        query = qr_ref[own]
        near = jnp.where(mask, times_transposed(query, kr_ref[own]), NEGATIVE)
        row_max = jnp.max(near, axis=-1, keepdims=True)
        if seen:
            past = pl.ds(start, seen)
            far = times_transposed(query, kr_ref[past])
            row_max = jnp.maximum(row_max, jnp.max(far, axis=-1, keepdims=True))
        near = jnp.exp2((near - row_max) * factor)
        total = jnp.sum(near, axis=-1, keepdims=True)
        context = times_plain(near.astype(jnp.bfloat16), vl_ref[own])
        if seen:
            far = jnp.exp2((far - row_max) * factor)
            total = total + jnp.sum(far, axis=-1, keepdims=True)
            context = context + times_plain(far.astype(jnp.bfloat16), vl_ref[past])
        ctx_ref[own] = (context / total).astype(jnp.bfloat16)
        norm_ref[0, own] = row_max * factor + jnp.log2(total)


def attend(qkv, scales, gain_query, gain_key, cosine, sine, start):
    rows = qkv.shape[0]
    width = qkv.shape[1] // 3
    heads = width // HD

    def column(shift):
        return pl.BlockSpec((rows, HD), lambda h, s: (0, h + shift))

    whole = lambda h, s: (0, 0)
    gain_spec = pl.BlockSpec((1, HD), lambda h, s: (0, h))
    low = jax.ShapeDtypeStruct((rows, width), jnp.bfloat16)
    pairs = rows * rows * width * 4 // 2
    return pl.pallas_call(
        attend_kernel,
        grid_spec=pltpu.PrefetchScalarGridSpec(
            num_scalar_prefetch=1,
            grid=(heads,),
            in_specs=[
                column(0),
                column(heads),
                column(2 * heads),
                pl.BlockSpec((rows, 2), whole),
                gain_spec,
                gain_spec,
                pl.BlockSpec((rows, HD), whole),
                pl.BlockSpec((rows, HD), whole),
            ],
            out_specs=[column(0)] * 4 + [pl.BlockSpec((1, rows, 1), lambda h, s: (h, 0, 0))],
        ),
        out_shape=[low] * 4 + [jax.ShapeDtypeStruct((heads, rows, 1), jnp.float32)],
        compiler_params=pltpu.CompilerParams(vmem_limit_bytes=kernel_vmem),
        cost_estimate=pl.CostEstimate(
            flops=pairs, bytes_accessed=rows * width * 24, transcendentals=pairs // 512
        ),
    )(start, qkv, qkv, qkv, scales, gain_query[None], gain_key[None], cosine, sine)


def attend_back_kernel(
    start_ref, qr_ref, kr_ref, vl_ref, dc_ref, norm_ref, q_ref, k_ref, scale_ref, gain_q_ref,
    gain_k_ref, cos_ref, sin_ref, dq_ref, dk_ref, dv_ref, inner_ref, gains_ref, key_acc, value_acc,
):
    rows = q_ref.shape[0]
    plain = HD ** (-0.5)
    factor = plain * LOG2_E
    start = pl.multiple_of(start_ref[0], CLEN)
    mask = diagonal()

    @pl.when(pl.program_id(0) == 0)
    def _():
        inner_ref[...] = jnp.zeros_like(inner_ref)

    key_acc[...] = jnp.zeros_like(key_acc)
    value_acc[...] = jnp.zeros_like(value_acc)

    def finish(values, part, raw_ref, column, gain_ref):
        back = turn(values * plain, cos_ref[part], -sin_ref[part])
        raw = raw_ref[part]
        scaled = back * gain_ref[...]
        inner_ref[part, column : column + 1] += jnp.sum(scaled * raw, axis=-1, keepdims=True)
        scale = scale_ref[part, column : column + 1]
        return scaled, jnp.sum(back * raw * scale, axis=0, keepdims=True)

    query_gain = jnp.zeros((1, HD), jnp.float32)
    for first, seen in block_plan(start, rows):
        own = pl.ds(first, CLEN)
        query = qr_ref[own]
        grad = dc_ref[own]
        norm = norm_ref[0, own]
        pieces = [(own, True)]
        if seen:
            pieces.append((pl.ds(start, seen), False))
        kept = []
        delta = jnp.zeros((CLEN, 1), jnp.float32)
        for part, near in pieces:
            probs = jnp.exp2(times_transposed(query, kr_ref[part]) * factor - norm)
            if near:
                probs = jnp.where(mask, probs, 0.0)
            prob_grad = times_transposed(grad, vl_ref[part])
            delta = delta + jnp.sum(probs * prob_grad, axis=-1, keepdims=True)
            kept.append((probs, prob_grad))
        query_grad = jnp.zeros((CLEN, HD), jnp.float32)
        for (part, near), (probs, prob_grad) in zip(pieces, kept):
            score_grad = (probs * (prob_grad - delta)).astype(jnp.bfloat16)
            query_grad = query_grad + times_plain(score_grad, kr_ref[part])
            key_acc[part] += transposed_times(score_grad, query)
            value_acc[part] += transposed_times(probs.astype(jnp.bfloat16), grad)
        scaled, gain_part = finish(query_grad, own, q_ref, 0, gain_q_ref)
        dq_ref[own] = scaled
        query_gain = query_gain + gain_part
    key_gain = jnp.zeros((1, HD), jnp.float32)
    for at in range(0, rows, CLEN):
        part = pl.ds(at, CLEN)
        scaled, gain_part = finish(key_acc[part], part, k_ref, 1, gain_k_ref)
        dk_ref[part] = scaled
        key_gain = key_gain + gain_part
        dv_ref[part] = value_acc[part].astype(jnp.bfloat16)
    gains_ref[...] = jnp.concatenate([query_gain, key_gain], axis=0)


def attend_back(
    query_rot, key_rot, value_low, context_grad, log_norm, qkv, scales, gain_query, gain_key,
    cosine, sine, start,
):
    rows, width = query_rot.shape
    heads = width // HD

    def column(shift):
        return pl.BlockSpec((rows, HD), lambda h, s: (0, h + shift))

    whole = lambda h, s: (0, 0)
    gain_spec = pl.BlockSpec((1, HD), lambda h, s: (0, h))
    full = jax.ShapeDtypeStruct((rows, width), jnp.float32)
    pairs = rows * rows * width * 10 // 2
    return pl.pallas_call(
        attend_back_kernel,
        grid_spec=pltpu.PrefetchScalarGridSpec(
            num_scalar_prefetch=1,
            grid=(heads,),
            in_specs=[column(0)] * 4
            + [
                pl.BlockSpec((1, rows, 1), lambda h, s: (h, 0, 0)),
                column(0),
                column(heads),
                pl.BlockSpec((rows, 2), whole),
                gain_spec,
                gain_spec,
                pl.BlockSpec((rows, HD), whole),
                pl.BlockSpec((rows, HD), whole),
            ],
            out_specs=[
                column(0),
                column(0),
                column(0),
                pl.BlockSpec((rows, 2), whole),
                pl.BlockSpec((2, HD), lambda h, s: (0, h)),
            ],
            scratch_shapes=[pltpu.VMEM((rows, HD), jnp.float32)] * 2,
        ),
        out_shape=[
            full,
            full,
            jax.ShapeDtypeStruct((rows, width), jnp.bfloat16),
            jax.ShapeDtypeStruct((rows, 2), jnp.float32),
            jax.ShapeDtypeStruct((2, width), jnp.float32),
        ],
        compiler_params=pltpu.CompilerParams(vmem_limit_bytes=kernel_vmem),
        cost_estimate=pl.CostEstimate(
            flops=pairs, bytes_accessed=rows * width * 34, transcendentals=pairs // 1280
        ),
    )(
        start, query_rot, key_rot, value_low, context_grad, log_norm, qkv, qkv, scales,
        gain_query[None], gain_key[None], cosine, sine,
    )


def swap(values, distance, count):
    pairs = [(at, at ^ distance) for at in range(count)]
    return lax.ppermute(values, "col", pairs)


def exchange(pieces, count):
    return [pieces[0]] + [swap(pieces[d], d, count) for d in range(1, count)]


def spread(values, count):
    return [values] + [swap(values, d, count) for d in range(1, count)]


def in_order(pieces, me, axis):
    pieces = list(pieces)
    count = len(pieces)
    bit = 1
    while bit < count:
        chosen = (me & bit) != 0
        pieces = [
            jnp.where(chosen, pieces[at ^ bit], pieces[at]) for at in range(count)
        ]
        bit *= 2
    return jnp.concatenate(pieces, axis=axis)


def total_over_col(values, count):
    got = spread(values, count)
    total = got[0]
    for piece in got[1:]:
        total = total + piece
    return total


def owned_sum(pieces, count):
    got = exchange([pieces[0]] + [p.astype(jnp.bfloat16) for p in pieces[1:]], count)
    total = got[0]
    for piece in got[1:]:
        total = total + piece.astype(jnp.float32)
    return total


def body(
    tokens,
    weight_query,
    weight_key,
    weight_value,
    weight_output,
    weight_gate,
    weight_up,
    weight_down,
    gain_query,
    gain_key,
    gain_attention,
    gain_feedforward,
    positions,
    segments,
    cotangent,
):
    row_count, col_width = tokens.shape
    count = D // col_width
    own_rows = row_count // count
    me = lax.axis_index("col")
    col_start = me * col_width

    def rows_of(values, d):
        return lax.dynamic_slice_in_dim(values, (me ^ d) * own_rows, own_rows, 0)

    def cols_of(values, d):
        return lax.dynamic_slice_in_dim(values, (me ^ d) * col_width, col_width, 1)

    def share_rows(values, axis):
        return lax.psum_scatter(values, "row", scatter_dimension=axis, tiled=True).astype(
            jnp.float32
        )

    def block(values, d):
        return values[d * own_rows : (d + 1) * own_rows]

    features = in_order(spread(tokens, count), me, 1)
    qkv_matrix = lax.all_gather(
        jnp.concatenate([weight_query, weight_key, weight_value], axis=1), "row", axis=0, tiled=True
    )
    output_matrix = lax.all_gather(weight_output, "row", axis=1, tiled=True)
    gate_matrix = lax.all_gather(weight_gate, "row", axis=0, tiled=True)
    up_matrix = lax.all_gather(weight_up, "row", axis=0, tiled=True)
    down_matrix = lax.all_gather(weight_down, "row", axis=1, tiled=True)

    qkv = times_plain(features, qkv_matrix)
    query_raw = qkv[:, :col_width]
    key_raw = qkv[:, col_width : 2 * col_width]
    square_sums = total_over_col(
        jnp.stack([jnp.sum(query_raw * query_raw, axis=-1), jnp.sum(key_raw * key_raw, axis=-1)]),
        count,
    )
    scales = lax.rsqrt(square_sums / D + EPSILON).T
    cosine_table, sine_table = rotation(positions)
    start = jnp.min(
        jnp.where(segments == 0, jnp.arange(row_count, dtype=jnp.int32), row_count)
    ).reshape(1)
    query_rot, key_rot, value_low, context_low, log_norm = attend(
        qkv, scales, gain_query, gain_key, cosine_table, sine_table, start
    )
    upstream_low = in_order(
        exchange([rows_of(cotangent, d) for d in range(count)], count), me, 1
    )
    context_low, upstream_low = lax.optimization_barrier((context_low, upstream_low))
    attention_out = owned_sum(
        [times_plain(rows_of(context_low, d), output_matrix) for d in range(count)], count
    )
    attention_scale = lax.rsqrt(
        jnp.mean(attention_out * attention_out, axis=-1, keepdims=True) + EPSILON
    )
    hidden_state = (
        rows_of(features, 0).astype(jnp.float32) + attention_out * attention_scale * gain_attention
    )
    hidden_low = jnp.concatenate(spread(hidden_state.astype(jnp.bfloat16), count), axis=0)
    gate = times_plain(hidden_low, gate_matrix)
    up_rows = times_plain(hidden_low, up_matrix)
    sigmoid_gate = jax.nn.sigmoid(gate)
    silu_gate = gate * sigmoid_gate
    activated = (silu_gate * up_rows).astype(jnp.bfloat16)
    feedforward_out = owned_sum(
        [times_plain(block(activated, d), down_matrix) for d in range(count)], count
    )
    feedforward_scale = lax.rsqrt(
        jnp.mean(feedforward_out * feedforward_out, axis=-1, keepdims=True) + EPSILON
    )
    result = (
        hidden_state + feedforward_out * feedforward_scale * gain_feedforward
    ).astype(jnp.bfloat16)
    activations = in_order(exchange([cols_of(result, d) for d in range(count)], count), me, 0)
    upstream = upstream_low.astype(jnp.float32)
    feedforward_own_grad, feedforward_gain_part = norm_back(
        upstream, feedforward_out, feedforward_scale, gain_feedforward
    )
    feedforward_grad = jnp.concatenate(
        spread(feedforward_own_grad.astype(jnp.bfloat16), count), axis=0
    )
    down_weight_part = transposed_times(activated, feedforward_grad).astype(jnp.bfloat16)
    feedforward_grad, down_weight_part = lax.optimization_barrier(
        (feedforward_grad, down_weight_part)
    )
    down_weight_grad = share_rows(down_weight_part, 1)
    activated_grad = times_transposed(feedforward_grad, down_matrix)
    gate_grad = (
        activated_grad * up_rows * sigmoid_gate * (1.0 + gate * (1.0 - sigmoid_gate))
    ).astype(jnp.bfloat16)
    up_grad = (activated_grad * silu_gate).astype(jnp.bfloat16)
    hidden_grad = (
        owned_sum(
            [
                times_transposed(block(gate_grad, d), gate_matrix)
                + times_transposed(block(up_grad, d), up_matrix)
                for d in range(count)
            ],
            count,
        )
        + upstream
    )
    gate_weight_part = transposed_times(hidden_low, gate_grad).astype(jnp.bfloat16)
    up_weight_part = transposed_times(hidden_low, up_grad).astype(jnp.bfloat16)
    attention_own_grad, attention_gain_part = norm_back(
        hidden_grad, attention_out, attention_scale, gain_attention
    )
    attention_own_low, gate_weight_part = lax.optimization_barrier(
        (attention_own_grad.astype(jnp.bfloat16), gate_weight_part)
    )
    gate_weight_grad = share_rows(gate_weight_part, 0)
    attention_grad = in_order(spread(attention_own_low, count), me, 0)
    attention_grad, up_weight_part, down_weight_grad = lax.optimization_barrier(
        (attention_grad, up_weight_part, down_weight_grad)
    )
    up_weight_grad = share_rows(up_weight_part, 0)
    residual_low = hidden_grad.astype(jnp.bfloat16)
    residual_low = in_order(
        exchange([cols_of(residual_low, d) for d in range(count)], count), me, 0
    )
    context_grad = times_transposed(attention_grad, output_matrix).astype(jnp.bfloat16)
    output_weight_part = transposed_times(context_low, attention_grad).astype(jnp.bfloat16)
    context_grad, output_weight_part = lax.optimization_barrier((context_grad, output_weight_part))
    output_weight_grad = share_rows(output_weight_part, 1)
    query_scaled, key_scaled, value_grad, inner_parts, gain_parts = attend_back(
        query_rot, key_rot, value_low, context_grad, log_norm, qkv, scales, gain_query, gain_key,
        cosine_table, sine_table, start,
    )
    inner_parts, residual_low, activations, gate_weight_grad = lax.optimization_barrier(
        (inner_parts, residual_low, activations, gate_weight_grad)
    )
    residual_grad = residual_low.astype(jnp.float32)
    inner_sums = total_over_col(inner_parts.T, count) / D
    query_scale, key_scale = scales[:, 0:1], scales[:, 1:2]
    query_raw_grad = (
        query_scale * query_scaled
        - query_raw * query_scale * query_scale * query_scale * inner_sums[0][:, None]
    ).astype(jnp.bfloat16)
    key_raw_grad = (
        key_scale * key_scaled
        - key_raw * key_scale * key_scale * key_scale * inner_sums[1][:, None]
    ).astype(jnp.bfloat16)
    qkv_grad = jnp.concatenate([query_raw_grad, key_raw_grad, value_grad], axis=1)
    qkv_weight_part = transposed_times(features, qkv_grad).astype(jnp.bfloat16)
    input_grad = (
        owned_sum(
            [
                times_transposed(
                    qkv_grad,
                    lax.dynamic_slice_in_dim(qkv_matrix, (me ^ d) * col_width, col_width, 0),
                )
                for d in range(count)
            ],
            count,
        )
        + residual_grad
    )

    qkv_weight_grad = share_rows(qkv_weight_part, 0)
    gain_totals = lax.psum(
        (
            spread_share(gain_parts[0], col_start),
            spread_share(gain_parts[1], col_start),
            attention_gain_part,
            feedforward_gain_part,
        ),
        ("row", "col"),
    )
    query_gain_grad = lax.dynamic_slice_in_dim(gain_totals[0], col_start, col_width, 0)
    key_gain_grad = lax.dynamic_slice_in_dim(gain_totals[1], col_start, col_width, 0)
    return (
        activations,
        input_grad,
        qkv_weight_grad[:, :col_width],
        qkv_weight_grad[:, col_width : 2 * col_width],
        qkv_weight_grad[:, 2 * col_width :],
        output_weight_grad,
        gate_weight_grad,
        up_weight_grad,
        down_weight_grad,
        query_gain_grad,
        key_gain_grad,
        gain_totals[2],
        gain_totals[3],
    )


def solution(mesh):
    in_specs = (
        P("row", "col"),
        P("row", "col"),
        P("row", "col"),
        P("row", "col"),
        P("col", "row"),
        P("row", "col"),
        P("row", "col"),
        P("col", "row"),
        P("col"),
        P("col"),
        P(),
        P(),
        P("row"),
        P("row"),
        P("row", "col"),
    )
    out_specs = (
        P("row", "col"),
        P("row", "col"),
        P("row", "col"),
        P("row", "col"),
        P("row", "col"),
        P("col", "row"),
        P("row", "col"),
        P("row", "col"),
        P("col", "row"),
        P("col"),
        P("col"),
        P(),
        P(),
    )
    return jax.shard_map(body, mesh=mesh, in_specs=in_specs, out_specs=out_specs, check_vma=False)
```

```python
import jax
import jax.numpy as jnp
from jax import lax
from jax.experimental import pallas as pl
from jax.experimental.pallas import tpu as pltpu
from jax.sharding import PartitionSpec as P

D = 2048
HD = 128


EPSILON = 1e-06
ROPE_BASE = 500000.0
NEGATIVE = -1e30


def times_plain(left, right):
    return jnp.dot(left, right, preferred_element_type=jnp.float32)


def times_transposed(left, right):
    return lax.dot_general(
        left, right, (((1,), (1,)), ((), ())), preferred_element_type=jnp.float32
    )


def transposed_times(left, right):
    return lax.dot_general(
        left, right, (((0,), (0,)), ((), ())), preferred_element_type=jnp.float32
    )


def rotation(positions):
    half_dim = HD // 2
    inverse = ROPE_BASE ** (-(jnp.arange(half_dim).astype(jnp.float32) * 2.0) / HD)
    angles = positions.astype(jnp.float32)[:, None] * inverse[None, :]
    cosine, sine = jnp.cos(angles), jnp.sin(angles)
    return (
        jnp.concatenate([cosine, cosine], axis=1),
        jnp.concatenate([-sine, sine], axis=1),
    )


def norm_back(incoming, values, norm_scale, gain_vector):
    scaled = gain_vector * incoming
    inner_mean = jnp.mean(scaled * values, axis=-1, keepdims=True)
    grad_values = norm_scale * scaled - values * norm_scale * norm_scale * norm_scale * inner_mean
    return (grad_values, jnp.sum(incoming * values * norm_scale, axis=0))


PROMPT = 1024
CLEN = 256
LOG2_E = 1.4426950408889634
kernel_vmem = 40 * 1024 * 1024


def turn(values, cosine, sine):
    return values * cosine + pltpu.roll(values, HD // 2, 1) * sine


def block_plan(start, rows):
    plan = [(start + at, at) for at in range(0, PROMPT, CLEN)]
    for at in range(0, rows - PROMPT, CLEN):
        plan.append((jnp.where(at < start, at, at + PROMPT), PROMPT))
    return [(pl.multiple_of(first, CLEN), seen) for first, seen in plan]


def diagonal():
    shape = (CLEN, CLEN)
    return lax.broadcasted_iota(jnp.int32, shape, 1) <= lax.broadcasted_iota(jnp.int32, shape, 0)


def attend_kernel(
    start_ref, q_ref, k_ref, v_ref, scale_ref, gain_q_ref, gain_k_ref, cos_ref, sin_ref,
    qr_ref, kr_ref, vl_ref, ctx_ref, norm_ref,
):
    rows = q_ref.shape[0]
    factor = HD ** (-0.5) * LOG2_E
    for at in range(0, rows, CLEN):
        part = pl.ds(at, CLEN)
        cosine, sine = cos_ref[part], sin_ref[part]
        scales = scale_ref[part]
        query = q_ref[part] * scales[:, 0:1] * gain_q_ref[...]
        key = k_ref[part] * scales[:, 1:2] * gain_k_ref[...]
        qr_ref[part] = turn(query, cosine, sine).astype(jnp.bfloat16)
        kr_ref[part] = turn(key, cosine, sine).astype(jnp.bfloat16)
        vl_ref[part] = v_ref[part].astype(jnp.bfloat16)
    start = pl.multiple_of(start_ref[0], CLEN)
    mask = diagonal()
    for first, seen in block_plan(start, rows):
        own = pl.ds(first, CLEN)
        query = qr_ref[own]
        near = jnp.where(mask, times_transposed(query, kr_ref[own]), NEGATIVE)
        row_max = jnp.max(near, axis=-1, keepdims=True)
        if seen:
            past = pl.ds(start, seen)
            far = times_transposed(query, kr_ref[past])
            row_max = jnp.maximum(row_max, jnp.max(far, axis=-1, keepdims=True))
        near = jnp.exp2((near - row_max) * factor)
        total = jnp.sum(near, axis=-1, keepdims=True)
        context = times_plain(near.astype(jnp.bfloat16), vl_ref[own])
        if seen:
            far = jnp.exp2((far - row_max) * factor)
            total = total + jnp.sum(far, axis=-1, keepdims=True)
            context = context + times_plain(far.astype(jnp.bfloat16), vl_ref[past])
        ctx_ref[own] = (context / total).astype(jnp.bfloat16)
        norm_ref[0, own] = row_max * factor + jnp.log2(total)


def attend(qkv, scales, gain_query, gain_key, cosine, sine, start):
    rows = qkv.shape[0]
    width = qkv.shape[1] // 3
    heads = width // HD

    def column(shift):
        return pl.BlockSpec((rows, HD), lambda h, s: (0, h + shift))

    whole = lambda h, s: (0, 0)
    gain_spec = pl.BlockSpec((1, HD), lambda h, s: (0, h))
    low = jax.ShapeDtypeStruct((rows, width), jnp.bfloat16)
    pairs = rows * rows * width * 4 // 2
    return pl.pallas_call(
        attend_kernel,
        grid_spec=pltpu.PrefetchScalarGridSpec(
            num_scalar_prefetch=1,
            grid=(heads,),
            in_specs=[
                column(0),
                column(heads),
                column(2 * heads),
                pl.BlockSpec((rows, 2), whole),
                gain_spec,
                gain_spec,
                pl.BlockSpec((rows, HD), whole),
                pl.BlockSpec((rows, HD), whole),
            ],
            out_specs=[column(0)] * 4 + [pl.BlockSpec((1, rows, 1), lambda h, s: (h, 0, 0))],
        ),
        out_shape=[low] * 4 + [jax.ShapeDtypeStruct((heads, rows, 1), jnp.float32)],
        compiler_params=pltpu.CompilerParams(vmem_limit_bytes=kernel_vmem),
        cost_estimate=pl.CostEstimate(
            flops=pairs, bytes_accessed=rows * width * 24, transcendentals=pairs // 512
        ),
    )(start, qkv, qkv, qkv, scales, gain_query[None], gain_key[None], cosine, sine)


def attend_back_kernel(
    start_ref, qr_ref, kr_ref, vl_ref, dc_ref, norm_ref, q_ref, k_ref, scale_ref, gain_q_ref,
    gain_k_ref, cos_ref, sin_ref, dq_ref, dk_ref, dv_ref, inner_ref, gains_ref, key_acc, value_acc,
):
    rows = q_ref.shape[0]
    plain = HD ** (-0.5)
    factor = plain * LOG2_E
    start = pl.multiple_of(start_ref[0], CLEN)
    mask = diagonal()

    @pl.when(pl.program_id(0) == 0)
    def _():
        inner_ref[...] = jnp.zeros_like(inner_ref)

    key_acc[...] = jnp.zeros_like(key_acc)
    value_acc[...] = jnp.zeros_like(value_acc)

    def finish(values, part, raw_ref, column, gain_ref):
        back = turn(values * plain, cos_ref[part], -sin_ref[part])
        raw = raw_ref[part]
        scaled = back * gain_ref[...]
        inner_ref[part, column : column + 1] += jnp.sum(scaled * raw, axis=-1, keepdims=True)
        scale = scale_ref[part, column : column + 1]
        return scaled, jnp.sum(back * raw * scale, axis=0, keepdims=True)

    query_gain = jnp.zeros((1, HD), jnp.float32)
    for first, seen in block_plan(start, rows):
        own = pl.ds(first, CLEN)
        query = qr_ref[own]
        grad = dc_ref[own]
        norm = norm_ref[0, own]
        pieces = [(own, True)]
        if seen:
            pieces.append((pl.ds(start, seen), False))
        kept = []
        delta = jnp.zeros((CLEN, 1), jnp.float32)
        for part, near in pieces:
            probs = jnp.exp2(times_transposed(query, kr_ref[part]) * factor - norm)
            if near:
                probs = jnp.where(mask, probs, 0.0)
            prob_grad = times_transposed(grad, vl_ref[part])
            delta = delta + jnp.sum(probs * prob_grad, axis=-1, keepdims=True)
            kept.append((probs, prob_grad))
        query_grad = jnp.zeros((CLEN, HD), jnp.float32)
        for (part, near), (probs, prob_grad) in zip(pieces, kept):
            score_grad = (probs * (prob_grad - delta)).astype(jnp.bfloat16)
            query_grad = query_grad + times_plain(score_grad, kr_ref[part])
            key_acc[part] += transposed_times(score_grad, query)
            value_acc[part] += transposed_times(probs.astype(jnp.bfloat16), grad)
        scaled, gain_part = finish(query_grad, own, q_ref, 0, gain_q_ref)
        dq_ref[own] = scaled
        query_gain = query_gain + gain_part
    key_gain = jnp.zeros((1, HD), jnp.float32)
    for at in range(0, rows, CLEN):
        part = pl.ds(at, CLEN)
        scaled, gain_part = finish(key_acc[part], part, k_ref, 1, gain_k_ref)
        dk_ref[part] = scaled
        key_gain = key_gain + gain_part
        dv_ref[part] = value_acc[part].astype(jnp.bfloat16)
    gains_ref[...] = jnp.concatenate([query_gain, key_gain], axis=0)


def attend_back(
    query_rot, key_rot, value_low, context_grad, log_norm, qkv, scales, gain_query, gain_key,
    cosine, sine, start,
):
    rows, width = query_rot.shape
    heads = width // HD

    def column(shift):
        return pl.BlockSpec((rows, HD), lambda h, s: (0, h + shift))

    whole = lambda h, s: (0, 0)
    gain_spec = pl.BlockSpec((1, HD), lambda h, s: (0, h))
    full = jax.ShapeDtypeStruct((rows, width), jnp.float32)
    pairs = rows * rows * width * 10 // 2
    return pl.pallas_call(
        attend_back_kernel,
        grid_spec=pltpu.PrefetchScalarGridSpec(
            num_scalar_prefetch=1,
            grid=(heads,),
            in_specs=[column(0)] * 4
            + [
                pl.BlockSpec((1, rows, 1), lambda h, s: (h, 0, 0)),
                column(0),
                column(heads),
                pl.BlockSpec((rows, 2), whole),
                gain_spec,
                gain_spec,
                pl.BlockSpec((rows, HD), whole),
                pl.BlockSpec((rows, HD), whole),
            ],
            out_specs=[
                column(0),
                column(0),
                column(0),
                pl.BlockSpec((rows, 2), whole),
                pl.BlockSpec((2, HD), lambda h, s: (0, h)),
            ],
            scratch_shapes=[pltpu.VMEM((rows, HD), jnp.float32)] * 2,
        ),
        out_shape=[
            full,
            full,
            jax.ShapeDtypeStruct((rows, width), jnp.bfloat16),
            jax.ShapeDtypeStruct((rows, 2), jnp.float32),
            jax.ShapeDtypeStruct((2, width), jnp.float32),
        ],
        compiler_params=pltpu.CompilerParams(vmem_limit_bytes=kernel_vmem),
        cost_estimate=pl.CostEstimate(
            flops=pairs, bytes_accessed=rows * width * 34, transcendentals=pairs // 1280
        ),
    )(
        start, query_rot, key_rot, value_low, context_grad, log_norm, qkv, qkv, scales,
        gain_query[None], gain_key[None], cosine, sine,
    )


def swap(values, distance, count):
    pairs = [(at, at ^ distance) for at in range(count)]
    return lax.ppermute(values, "col", pairs)


def exchange(pieces, count):
    return [pieces[0]] + [swap(pieces[d], d, count) for d in range(1, count)]


def halves(values):
    middle = values.shape[0] // 2
    return values[:middle], values[middle:]


def spread(values, count):
    if count != 4:
        return [values] + [swap(values, d, count) for d in range(1, count)]
    top, low = halves(values)
    top_two = swap(top, 2, count)
    low_one = swap(low, 1, count)
    top_one = swap(top, 1, count)
    low_two = swap(low, 2, count)
    top_three = swap(top_two, 1, count)
    low_three = swap(low_one, 2, count)
    return [
        values,
        jnp.concatenate([top_one, low_one], axis=0),
        jnp.concatenate([top_two, low_two], axis=0),
        jnp.concatenate([top_three, low_three], axis=0),
    ]


def in_order(pieces, me, axis):
    pieces = list(pieces)
    count = len(pieces)
    bit = 1
    while bit < count:
        chosen = (me & bit) != 0
        pieces = [
            jnp.where(chosen, pieces[at ^ bit], pieces[at]) for at in range(count)
        ]
        bit *= 2
    return jnp.concatenate(pieces, axis=axis)


def total_over(values, axis, count):
    distance = 1
    while distance < count:
        pairs = [(at, at ^ distance) for at in range(count)]
        values = values + lax.ppermute(values, axis, pairs)
        distance *= 2
    return values


def total_over_col(values, count):
    got = exchange([values] * count, count)
    total = got[0]
    for piece in got[1:]:
        total = total + piece
    return total


def wide(values):
    return values.astype(jnp.float32)


def narrow(values):
    return values.astype(jnp.bfloat16)


def owned_sum(pieces, count):
    if count != 4:
        got = exchange([pieces[0]] + [narrow(p) for p in pieces[1:]], count)
        total = got[0]
        for piece in got[1:]:
            total = total + wide(piece)
        return total
    top_own, low_own = halves(pieces[0])
    top_one, low_one = halves(narrow(pieces[1]))
    top_two, low_two = halves(narrow(pieces[2]))
    top_far, low_far = halves(narrow(pieces[3]))
    top_pass = swap(top_far, 1, count)
    low_pass = swap(low_far, 2, count)
    top_got = swap(top_one, 1, count)
    low_got = swap(low_two, 2, count)
    top_last = swap(narrow(wide(top_two) + wide(top_pass)), 2, count)
    low_last = swap(narrow(wide(low_one) + wide(low_pass)), 1, count)
    return jnp.concatenate(
        [
            top_own + wide(top_got) + wide(top_last),
            low_own + wide(low_got) + wide(low_last),
        ],
        axis=0,
    )


def body(
    tokens,
    weight_query,
    weight_key,
    weight_value,
    weight_output,
    weight_gate,
    weight_up,
    weight_down,
    gain_query,
    gain_key,
    gain_attention,
    gain_feedforward,
    positions,
    segments,
    cotangent,
):
    row_count, col_width = tokens.shape
    count = D // col_width
    row_groups = D // weight_query.shape[0]
    own_rows = row_count // count
    me = lax.axis_index("col")

    def rows_of(values, d):
        return lax.dynamic_slice_in_dim(values, (me ^ d) * own_rows, own_rows, 0)

    def cols_of(values, d):
        return lax.dynamic_slice_in_dim(values, (me ^ d) * col_width, col_width, 1)

    hidden_width = weight_gate.shape[1]

    def share_rows(values, axis):
        return lax.psum_scatter(values, "row", scatter_dimension=axis, tiled=True).astype(
            jnp.float32
        )

    def block(values, d):
        return values[d * own_rows : (d + 1) * own_rows]

    features = in_order(spread(tokens, count), me, 1)
    first_matrix = lax.all_gather(
        jnp.concatenate([weight_query, weight_key, weight_value, weight_output.T], axis=1),
        "row",
        axis=0,
        tiled=True,
    )
    qkv_matrix = first_matrix[:, : 3 * col_width]
    output_turned = first_matrix[:, 3 * col_width :]
    pair_matrix = lax.all_gather(
        jnp.concatenate([weight_gate, weight_up], axis=1), "row", axis=0, tiled=True
    )
    gate_matrix = pair_matrix[:, :hidden_width]
    up_matrix = pair_matrix[:, hidden_width:]
    down_matrix = lax.all_gather(weight_down, "row", axis=1, tiled=True)

    qkv = times_plain(features, qkv_matrix)
    query_raw = qkv[:, :col_width]
    key_raw = qkv[:, col_width : 2 * col_width]
    square_sums = total_over_col(
        jnp.stack([jnp.sum(query_raw * query_raw, axis=-1), jnp.sum(key_raw * key_raw, axis=-1)]),
        count,
    )
    scales = lax.rsqrt(square_sums / D + EPSILON).T
    cosine_table, sine_table = rotation(positions)
    start = jnp.min(
        jnp.where(segments == 0, jnp.arange(row_count, dtype=jnp.int32), row_count)
    ).reshape(1)
    query_rot, key_rot, value_low, context_low, log_norm = attend(
        qkv, scales, gain_query, gain_key, cosine_table, sine_table, start
    )
    upstream_low = in_order(
        exchange([rows_of(cotangent, d) for d in range(count)], count), me, 1
    )
    context_low, upstream_low = lax.optimization_barrier((context_low, upstream_low))
    attention_out = owned_sum(
        [times_transposed(rows_of(context_low, d), output_turned) for d in range(count)], count
    )
    attention_scale = lax.rsqrt(
        jnp.mean(attention_out * attention_out, axis=-1, keepdims=True) + EPSILON
    )
    hidden_state = (
        rows_of(features, 0).astype(jnp.float32) + attention_out * attention_scale * gain_attention
    )
    hidden_low = jnp.concatenate(spread(hidden_state.astype(jnp.bfloat16), count), axis=0)
    gate = times_plain(hidden_low, gate_matrix)
    up_rows = times_plain(hidden_low, up_matrix)
    sigmoid_gate = jax.nn.sigmoid(gate)
    silu_gate = gate * sigmoid_gate
    activated = (silu_gate * up_rows).astype(jnp.bfloat16)
    feedforward_out = owned_sum(
        [times_plain(block(activated, d), down_matrix) for d in range(count)], count
    )
    feedforward_scale = lax.rsqrt(
        jnp.mean(feedforward_out * feedforward_out, axis=-1, keepdims=True) + EPSILON
    )
    result = (
        hidden_state + feedforward_out * feedforward_scale * gain_feedforward
    ).astype(jnp.bfloat16)
    upstream = upstream_low.astype(jnp.float32)
    feedforward_own_grad, feedforward_gain_part = norm_back(
        upstream, feedforward_out, feedforward_scale, gain_feedforward
    )
    feedforward_grad = jnp.concatenate(
        spread(feedforward_own_grad.astype(jnp.bfloat16), count), axis=0
    )
    down_weight_part = transposed_times(activated, feedforward_grad).astype(jnp.bfloat16)
    feedforward_grad, down_weight_part = lax.optimization_barrier(
        (feedforward_grad, down_weight_part)
    )
    down_weight_grad = share_rows(down_weight_part, 1)
    activated_grad = times_transposed(feedforward_grad, down_matrix)
    gate_grad = (
        activated_grad * up_rows * sigmoid_gate * (1.0 + gate * (1.0 - sigmoid_gate))
    ).astype(jnp.bfloat16)
    up_grad = (activated_grad * silu_gate).astype(jnp.bfloat16)
    hidden_grad = (
        owned_sum(
            [
                times_transposed(block(gate_grad, d), gate_matrix)
                + times_transposed(block(up_grad, d), up_matrix)
                for d in range(count)
            ],
            count,
        )
        + upstream
    )
    gate_weight_part = transposed_times(hidden_low, gate_grad).astype(jnp.bfloat16)
    gate_weight_grad = share_rows(gate_weight_part, 0)
    hidden_grad, _ = lax.optimization_barrier((hidden_grad, gate_weight_part))
    up_weight_part = transposed_times(hidden_low, up_grad).astype(jnp.bfloat16)
    attention_own_grad, attention_gain_part = norm_back(
        hidden_grad, attention_out, attention_scale, gain_attention
    )
    attention_grad = in_order(spread(attention_own_grad.astype(jnp.bfloat16), count), me, 0)
    up_weight_grad = share_rows(up_weight_part, 0)
    attention_grad, _, down_weight_grad = lax.optimization_barrier(
        (attention_grad, up_weight_part, down_weight_grad)
    )
    context_grad = times_plain(attention_grad, output_turned).astype(jnp.bfloat16)
    output_weight_part = transposed_times(context_low, attention_grad).astype(jnp.bfloat16)
    context_grad, output_weight_part, residual_low, token_gains, result = (
        lax.optimization_barrier(
            (
                context_grad,
                output_weight_part,
                hidden_grad.astype(jnp.bfloat16),
                jnp.stack([attention_gain_part, feedforward_gain_part]),
                result,
            )
        )
    )
    output_weight_grad = share_rows(output_weight_part, 1)
    residual_low = in_order(
        exchange([cols_of(residual_low, d) for d in range(count)], count), me, 0
    )
    activations = in_order(exchange([cols_of(result, d) for d in range(count)], count), me, 0)
    token_gains = total_over(total_over(token_gains, "col", count), "row", row_groups)
    query_scaled, key_scaled, value_grad, inner_parts, gain_parts = attend_back(
        query_rot, key_rot, value_low, context_grad, log_norm, qkv, scales, gain_query, gain_key,
        cosine_table, sine_table, start,
    )
    inner_parts, residual_low, activations, gate_weight_grad, token_gains = (
        lax.optimization_barrier(
            (inner_parts, residual_low, activations, gate_weight_grad, token_gains)
        )
    )
    residual_grad = residual_low.astype(jnp.float32)
    inner_sums = total_over_col(inner_parts.T, count) / D
    query_scale, key_scale = scales[:, 0:1], scales[:, 1:2]
    query_raw_grad = (
        query_scale * query_scaled
        - query_raw * query_scale * query_scale * query_scale * inner_sums[0][:, None]
    ).astype(jnp.bfloat16)
    key_raw_grad = (
        key_scale * key_scaled
        - key_raw * key_scale * key_scale * key_scale * inner_sums[1][:, None]
    ).astype(jnp.bfloat16)
    qkv_grad = jnp.concatenate([query_raw_grad, key_raw_grad, value_grad], axis=1)
    qkv_weight_part = transposed_times(features, qkv_grad).astype(jnp.bfloat16)
    input_grad = (
        owned_sum(
            [
                times_transposed(
                    qkv_grad,
                    lax.dynamic_slice_in_dim(qkv_matrix, (me ^ d) * col_width, col_width, 0),
                )
                for d in range(count)
            ],
            count,
        )
        + residual_grad
    )

    qkv_weight_grad = share_rows(qkv_weight_part, 0)
    head_gains = total_over(gain_parts, "row", row_groups)
    return (
        activations,
        input_grad,
        qkv_weight_grad[:, :col_width],
        qkv_weight_grad[:, col_width : 2 * col_width],
        qkv_weight_grad[:, 2 * col_width :],
        output_weight_grad,
        gate_weight_grad,
        up_weight_grad,
        down_weight_grad,
        head_gains[0],
        head_gains[1],
        token_gains[0],
        token_gains[1],
    )


def solution(mesh):
    in_specs = (
        P("row", "col"),
        P("row", "col"),
        P("row", "col"),
        P("row", "col"),
        P("col", "row"),
        P("row", "col"),
        P("row", "col"),
        P("col", "row"),
        P("col"),
        P("col"),
        P(),
        P(),
        P("row"),
        P("row"),
        P("row", "col"),
    )
    out_specs = (
        P("row", "col"),
        P("row", "col"),
        P("row", "col"),
        P("row", "col"),
        P("row", "col"),
        P("col", "row"),
        P("row", "col"),
        P("row", "col"),
        P("col", "row"),
        P("col"),
        P("col"),
        P(),
        P(),
    )
    return jax.shard_map(body, mesh=mesh, in_specs=in_specs, out_specs=out_specs, check_vma=False)
```
